256 devices in a mesh: dp: 32 (over y, z_lo, core), tensor: 8 (over z_hi, x).
Axes of the slice: x: 4, y: 4, z: 8 (z_hi: 2, z_lo: 4; z = z_hi * 4 + z_lo), core: 2. Of those that a mesh axis runs over, the one named last changes fastest.
Arguments:
- cand_ids: int32 [16384], P('dp'), may hold values from 0 to 128001, as said below
- val_ids: int32 [1024], P('dp'), may hold values from 0 to 128001, as said below
- inputs: bfloat16 [16384, 8192], P('dp', 'tensor'), may hold values from -6 to 6
- cotangent: bfloat16 [16384, 8192], P('dp'), may hold values from -6 to 6
- queries: bfloat16 [16384, 8192], P('dp', 'tensor'), may hold values from -16 to 16
- key_rows: bfloat16 [16384, 1024], P('dp', 'tensor'), may hold values from -16 to 16
- value_rows: bfloat16 [16384, 1024], P('dp', 'tensor'), may hold values from -6 to 6
- out_weight: bfloat16 [8192, 8192], P('tensor', 'dp'), may hold values from -0.0625 to 0.0625
- val_inputs: bfloat16 [1024, 8192], P('dp', 'tensor'), may hold values from -6 to 6
- val_cotangents: bfloat16 [1024, 8192], P('dp', 'tensor'), may hold values from -6 to 6
- val_attention: bfloat16 [1024, 8192], P('dp', 'tensor'), may hold values from -6 to 6
- val_query_grads: bfloat16 [1024, 8192], P('dp', 'tensor'), may hold values from -6 to 6
- val_keyvalue_grads: bfloat16 [1024, 2048], P('dp', 'tensor'), may hold values from -6 to 6
Outputs:
- scores: float32 [64, 4], P('dp')
The draws below stay inside these ranges and needn't reach their ends.
Inputs may be any that keep to these rules, and one draw needn't show every extreme that they name: `cand_ids`: each aligned run of 256 ids is one sequence: ids below 128001, then the padding id 128001 on at most 128 trailing positions. `val_ids`: each aligned run of 256 ids is one sequence: ids below 128001, then the padding id 128001 on at most 128 trailing positions.
All inputs are finite; a program needn't handle non-finite values.
Results may differ from the reference program's by a relative error of at most 0.02.
Values may be sent and summed in bfloat16 or wider, within the bound.
No kernel may reach another device: no remote copies, remote signals or barrier semaphores. Data moves between devices by JAX's collectives and lax.ppermute only.
A program may use at most 192 MiB of HBM per device.

```python
import math
import jax
import jax.numpy as jnp
from jax import lax

D = 8192
HEADS = 64
KV = 8
HD = 128
LEN = 256
VALS = 4
TOKENS = 16384
VTOKENS = 1024
N_TENSOR = 8


pad_token = 128001


def token_draw(key, total):
    seq_count = total // LEN
    lengths = jax.random.randint(jax.random.fold_in(key, 1), (seq_count, 1), LEN // 2, LEN + 1)
    word_ids = jax.random.randint(jax.random.fold_in(key, 2), (seq_count, LEN), 0, pad_token)
    position = jnp.arange(LEN)[None, :]
    return jnp.where(position < lengths, word_ids, pad_token).reshape(total).astype(jnp.int32)


def draw_cand_ids(key, part):
    return token_draw(jax.random.fold_in(key, 3), TOKENS)


def draw_val_ids(key, part):
    return token_draw(jax.random.fold_in(key, 4), VTOKENS)


def base_noise(key, shape):
    return jnp.clip(jax.random.normal(key, shape, jnp.float32), -6.0, 6.0)


def draw_queries(key, part):
    noise = base_noise(jax.random.fold_in(key, 21), (TOKENS, HEADS * HD))
    return noise.astype(jnp.bfloat16)


def draw_key_rows(key, part):
    noise = base_noise(jax.random.fold_in(key, 22), (TOKENS, KV * HD))
    return noise.astype(jnp.bfloat16)


def block_levels(key, extent, split, low, high):
    factor_of, own = 1.0, jax.random.fold_in(key, 6)
    for dim, shards_of in split:
        draws = jnp.exp(jax.random.uniform(jax.random.fold_in(own, dim), (shards_of,), jnp.float32, low / len(split), high / len(split)))
        factor_of = factor_of * jnp.repeat(draws, extent[dim] // shards_of).reshape([-1 if axis == dim else 1 for axis in range(len(extent))])
    return factor_of


def bell_draw(own_key, shape, width, bound, cuts=(), kind=jnp.bfloat16):
    level = block_levels(own_key, shape, cuts, -0.22, 0.18) if cuts else 1.0
    result = jax.random.normal(own_key, shape, jnp.float32) * width * level
    return jnp.minimum(jnp.maximum(result, -bound), bound).astype(kind)


def setup_inputs(seed: int = 0) -> dict:
    streams_of = jax.random.split(jax.random.key(seed), 14)
    cand_ids = draw_cand_ids(jax.random.fold_in(streams_of[13], 71), 0)
    val_ids = draw_val_ids(jax.random.fold_in(streams_of[13], 71), 0)
    inputs = bell_draw(streams_of[2], (TOKENS, D), 1.0, 6.0, ((0, 32), (1, 8)))
    cotangent = bell_draw(streams_of[3], (TOKENS, D), 1.0, 6.0, ((0, 32),))
    queries = draw_queries(jax.random.fold_in(streams_of[13], 71), 0)
    key_rows = draw_key_rows(jax.random.fold_in(streams_of[13], 71), 0)
    value_rows = bell_draw(streams_of[6], (TOKENS, KV * HD), 1.0, 6.0, ((0, 32), (1, 8)))
    out_weight = bell_draw(streams_of[7], (HEADS * HD, D), (HEADS * HD) ** -0.5, 0.0625, ((0, 8), (1, 32)))
    val_inputs = bell_draw(streams_of[8], (VTOKENS, D), 1.0, 6.0, ((0, 32), (1, 8)))
    val_cotangents = bell_draw(streams_of[9], (VTOKENS, D), 1.0, 6.0, ((0, 32), (1, 8)))
    val_attention = bell_draw(streams_of[10], (VTOKENS, HEADS * HD), 1.0, 6.0, ((0, 32), (1, 8)))
    val_query_grads = bell_draw(streams_of[11], (VTOKENS, HEADS * HD), 1.0, 6.0, ((0, 32), (1, 8)))
    val_keyvalue_grads = bell_draw(streams_of[12], (VTOKENS, 2 * KV * HD), 1.0, 6.0, ((0, 32), (1, 8)))
    return {"cand_ids": cand_ids, "val_ids": val_ids, "inputs": inputs, "cotangent": cotangent, "queries": queries, "key_rows": key_rows, "value_rows": value_rows, "out_weight": out_weight, "val_inputs": val_inputs, "val_cotangents": val_cotangents, "val_attention": val_attention, "val_query_grads": val_query_grads, "val_keyvalue_grads": val_keyvalue_grads}


pad_token = 128001
rope_base = 500000.0

def rotation(seq_len, head_width):
    half_dim = head_width // 2
    inv_freq = rope_base ** (-(jnp.arange(half_dim).astype(jnp.float32) * 2.0 / head_width))
    angles = jnp.arange(seq_len).astype(jnp.float32)[:, None] * inv_freq[None, :]
    angles = jnp.concatenate([angles, angles], axis=1)
    return (jnp.cos(angles), jnp.sin(angles))

def turn_half(features):
    half_dim = features.shape[-1] // 2
    return jnp.concatenate([-features[..., half_dim:], features[..., :half_dim]], axis=-1)

def rounded(features):
    return lax.optimization_barrier(features.astype(jnp.bfloat16)).astype(jnp.float32)

def sequence_pass(pieces):
    query_raw, key_raw, value_part, grad_out = pieces
    seq_len, head_width = (key_raw.shape[0], key_raw.shape[-1])
    cos_table, sine_table = rotation(seq_len, head_width)
    score_scale = 1.0 / math.sqrt(head_width)
    q_float = query_raw.astype(jnp.float32)
    k_float = key_raw.astype(jnp.float32)
    query_rot = rounded(q_float * cos_table[:, None, None, :] + turn_half(q_float) * sine_table[:, None, None, :])
    key_rot = rounded(k_float * cos_table[:, None, :] + turn_half(k_float) * sine_table[:, None, :])
    value_float = value_part.astype(jnp.float32)
    grad_float = grad_out.astype(jnp.float32)
    logits = jnp.einsum('lkgd,mkd->kglm', query_rot, key_rot) * score_scale
    allowed = jnp.arange(seq_len)[None, :] <= jnp.arange(seq_len)[:, None]
    logits = jnp.where(allowed, logits, -jnp.inf)
    row_max = lax.optimization_barrier(jnp.max(logits, axis=-1, keepdims=True))
    raised = jnp.exp(logits - row_max)
    attn_probs = raised / lax.optimization_barrier(jnp.sum(raised, axis=-1, keepdims=True))
    probs_low = rounded(attn_probs)
    attended = jnp.einsum('kglm,mkd->lkgd', probs_low, value_float).astype(jnp.bfloat16)
    prob_grad = jnp.einsum('lkgd,mkd->kglm', grad_float, value_float)
    row_delta = lax.optimization_barrier(jnp.sum(attn_probs * prob_grad, axis=-1, keepdims=True))
    logit_grad = rounded(attn_probs * (prob_grad - row_delta) * score_scale)
    dquery = jnp.einsum('kglm,mkd->lkgd', logit_grad, key_rot)
    key_grad = jnp.einsum('kglm,lkgd->mkd', logit_grad, query_rot)
    dvalue = jnp.einsum('kglm,lkgd->mkd', probs_low, grad_float)
    dquery_raw = (dquery * cos_table[:, None, None, :] - turn_half(dquery) * sine_table[:, None, None, :]).astype(jnp.bfloat16)
    dkey_raw = (key_grad * cos_table[:, None, :] - turn_half(key_grad) * sine_table[:, None, :]).astype(jnp.bfloat16)
    return (attended, dquery_raw, jnp.stack([dkey_raw, dvalue.astype(jnp.bfloat16)], axis=2))

def block_gram(left, right):
    return jnp.dot(left, right.T, preferred_element_type=jnp.float32)

def reference(cand_ids, val_ids, inputs, cotangent, queries, key_rows, value_rows, out_weight, val_inputs, val_cotangents, val_attention, val_query_grads, val_keyvalue_grads):
    head_group = HEADS // KV
    seq_count = TOKENS // LEN
    live_rows = (cand_ids != pad_token).astype(jnp.float32)[:, None]
    masked = (cotangent.astype(jnp.float32) * live_rows).astype(jnp.bfloat16)
    grad_attn = jnp.dot(masked, out_weight.T, preferred_element_type=jnp.float32).astype(jnp.bfloat16)
    q_split = queries.reshape(seq_count, LEN, KV, head_group, HD)
    k_split = key_rows.reshape(seq_count, LEN, KV, HD)
    v_split = value_rows.reshape(seq_count, LEN, KV, HD)
    g_split = grad_attn.reshape(seq_count, LEN, KV, head_group, HD)
    attended, dquery, kv_grads = lax.map(sequence_pass, (q_split, k_split, v_split, g_split))
    attended = attended.reshape(TOKENS, HEADS * HD)
    dquery = dquery.reshape(TOKENS, HEADS * HD)
    kv_grads = kv_grads.reshape(TOKENS, 2 * KV * HD)
    val_live = (val_ids != pad_token).astype(jnp.float32)[:, None]
    val_dy = (val_cotangents.astype(jnp.float32) * val_live).astype(jnp.bfloat16)
    val_dq = (val_query_grads.astype(jnp.float32) * val_live).astype(jnp.bfloat16)
    val_dkv = (val_keyvalue_grads.astype(jnp.float32) * val_live).astype(jnp.bfloat16)
    d_block = D // N_TENSOR
    h_block = HEADS * HD // N_TENSOR
    k_block = 2 * KV * HD // N_TENSOR
    gram_attn = jnp.zeros((TOKENS, VTOKENS), jnp.float32)
    gram_cot = jnp.zeros((TOKENS, VTOKENS), jnp.float32)
    gram_input = jnp.zeros((TOKENS, VTOKENS), jnp.float32)
    gram_proj = jnp.zeros((TOKENS, VTOKENS), jnp.float32)
    for tensor_part in range(N_TENSOR):
        d_cut = slice(tensor_part * d_block, (tensor_part + 1) * d_block)
        h_cut = slice(tensor_part * h_block, (tensor_part + 1) * h_block)
        k_cut = slice(tensor_part * k_block, (tensor_part + 1) * k_block)
        gram_attn = gram_attn + rounded(block_gram(attended[:, h_cut], val_attention[:, h_cut]))
        gram_cot = gram_cot + rounded(block_gram(masked[:, d_cut], val_dy[:, d_cut]))
        gram_input = gram_input + rounded(block_gram(inputs[:, d_cut], val_inputs[:, d_cut]))
        gram_proj = gram_proj + rounded(block_gram(dquery[:, h_cut], val_dq[:, h_cut]) + block_gram(kv_grads[:, k_cut], val_dkv[:, k_cut]))
    product = gram_attn * gram_cot + gram_input * gram_proj
    return lax.optimization_barrier(jnp.sum(product.reshape(seq_count, LEN, VALS, LEN), axis=(1, 3))) * (1.0 / (64.0 * D))
```

```python
import functools
import math

import jax
import jax.numpy as jnp
from jax import lax
from jax.experimental import pallas as pl
from jax.experimental.pallas import tpu as pltpu
from jax.sharding import Mesh
from jax.sharding import PartitionSpec as P

D = 8192
HEADS = 64
KV = 8
HD = 128
LEN = 256
VALS = 4
GROUP = HEADS // KV
DP = ("y", "z", "c")
TENSOR = ("h", "x")
pad_token = 128001
rope_base = 500000.0
SCALE = 1.0 / math.sqrt(HD)


def shift(x, axis, step):
    n = lax.axis_size(axis)
    return lax.ppermute(x, axis, [(i, (i + step) % n) for i in range(n)])


def swap(x):
    return lax.ppermute(x, "c", [(0, 1), (1, 0)])


def along_y(block, onward):
    below = shift(block, "y", 1)
    above = shift(block, "y", -1)
    far = shift(below if onward > 0 else above, "y", onward)
    return block, below, above, far


def along_z(block):
    blocks = [block]
    for _ in range(1, 4):
        blocks.append(shift(blocks[-1], "z", 1))
    return blocks


COLS, AHEAD, BEHIND, FEATURE = 0, 16, 20, 24


def positions():
    y, z, c = (lax.axis_index(a) for a in DP)
    x, tensor = lax.axis_index("x"), lax.axis_index(TENSOR)
    k = jnp.arange(32, dtype=jnp.int32)
    slot = k // 4
    dy = jnp.where(k % 4 == 1, 3, jnp.where(k % 4 == 2, 1, jnp.where(k % 4 == 3, 2, 0)))
    cols = ((y + dy) % 4 * 4 + (z + 4 - slot) % 4) * 2 + c
    ahead, behind = (x + k) % 4, (x + 8 - k % 4) % 4
    at = jnp.where(k < AHEAD, cols, jnp.where(k < BEHIND, ahead, behind))
    return jnp.where(k == FEATURE, tensor, at).astype(jnp.int32)


def limited(mib):
    return pltpu.CompilerParams(vmem_limit_bytes=mib << 20)


def nt_dot(left, right):
    return lax.dot_general(
        left, right, (((1,), (1,)), ((), ())), preferred_element_type=jnp.float32
    )


def tn_dot(left, right):
    return lax.dot_general(
        left, right, (((0,), (0,)), ((), ())), preferred_element_type=jnp.float32
    )


def project_kernel(has_sum, at_ref, *refs):
    own, other, blocks = refs[:4], refs[4:8], refs[8:12]
    weight = jnp.concatenate([r[...] for r in blocks], axis=1)
    outs = refs[-2:]
    sums = refs[12:14] if has_sum else (None, None)
    for side, out, total in zip((own, other), outs, sums):
        left = jnp.concatenate([r[...] for r in side], axis=1)
        part = nt_dot(left, weight)
        out[...] = part if total is None else total[...] + part


def project(own, other, at, slot, blocks, sums):
    rows, tile = own.shape[0], 256
    heads, width = blocks[0].shape

    def at_block(k):
        return pl.BlockSpec((tile, width), lambda i, t: (i, t[COLS + 4 * slot + k]))

    whole = [pl.BlockSpec(b.shape, lambda i, t: (0, 0)) for b in blocks]
    tiles = [pl.BlockSpec((tile, heads), lambda i, t: (i, 0))] * 2
    shape = jax.ShapeDtypeStruct((rows, heads), jnp.float32)
    return pl.pallas_call(
        functools.partial(project_kernel, sums is not None),
        grid_spec=pltpu.PrefetchScalarGridSpec(
            num_scalar_prefetch=1,
            grid=(rows // tile,),
            in_specs=[at_block(k) for k in range(4)] * 2
            + whole
            + (tiles if sums is not None else []),
            out_specs=tiles,
        ),
        out_shape=[shape, shape],
        input_output_aliases={13: 0, 14: 1} if sums is not None else {},
        compiler_params=limited(18),
    )(at, *([own] * 4), *([other] * 4), *blocks, *(sums or ()))


def turned(u):
    return pltpu.roll(u, HD // 2, 1)


def rotated(ref_value, cos, sine):
    u = ref_value.astype(jnp.float32)
    return (u * cos + turned(u) * sine).astype(jnp.bfloat16)


EXP_SCALE = SCALE * math.log2(math.e)


def forward_kernel(q_ref, k_ref, v_ref, cos_ref, sine_ref, live_ref, out_ref):
    cos, sine = cos_ref[...], sine_ref[...]
    live = live_ref[...]
    k_rot = rotated(k_ref[...], cos, sine)
    values = v_ref[...]
    rows = lax.broadcasted_iota(jnp.int32, (LEN, LEN), 0)
    allowed = lax.broadcasted_iota(jnp.int32, (LEN, LEN), 1) <= rows
    for g in range(GROUP):
        span = slice(g * HD, (g + 1) * HD)
        q_rot = rotated(q_ref[:, span], cos, sine)
        logits = jnp.where(allowed, nt_dot(q_rot, k_rot), -jnp.inf)
        raised = jnp.exp2((logits - jnp.max(logits, axis=1, keepdims=True)) * EXP_SCALE)
        low = (raised * (1.0 / jnp.sum(raised, axis=1, keepdims=True))).astype(jnp.bfloat16)
        attended = jnp.dot(low, values, preferred_element_type=jnp.float32)
        out_ref[:, span] = (attended * live).astype(jnp.bfloat16)


def backward_kernel(
    q_ref, k_ref, v_ref, cos_ref, sine_ref, mine_ref, recv_ref, live_ref, out_ref
):
    cos, sine = cos_ref[...], sine_ref[...]
    k_rot = rotated(k_ref[...], cos, sine)
    values = v_ref[...]
    keys = lax.broadcasted_iota(jnp.int32, (LEN, LEN), 0)
    allowed = keys <= lax.broadcasted_iota(jnp.int32, (LEN, LEN), 1)
    live = live_ref[...]
    dkey = jnp.zeros((LEN, HD), jnp.float32)
    dvalue = jnp.zeros((LEN, HD), jnp.float32)
    for g in range(GROUP):
        span = slice(g * HD, (g + 1) * HD)
        grad = ((mine_ref[:, span] + recv_ref[:, span]) * live).astype(jnp.bfloat16)
        q_rot = rotated(q_ref[:, span], cos, sine)
        logits = jnp.where(allowed, nt_dot(k_rot, q_rot), -jnp.inf)
        raised = jnp.exp2((logits - jnp.max(logits, axis=0, keepdims=True)) * EXP_SCALE)
        probs = raised * (1.0 / jnp.sum(raised, axis=0, keepdims=True))
        low = probs.astype(jnp.bfloat16)
        dprob = nt_dot(values, grad)
        delta = jnp.sum(probs * dprob, axis=0, keepdims=True)
        dlogit = (probs * (dprob - delta)).astype(jnp.bfloat16)
        dquery = tn_dot(dlogit, k_rot)
        dkey = dkey + jnp.dot(dlogit, q_rot, preferred_element_type=jnp.float32)
        dvalue = dvalue + jnp.dot(low, grad, preferred_element_type=jnp.float32)
        dquery = dquery * SCALE
        out_ref[:, span] = (dquery * cos - turned(dquery) * sine).astype(jnp.bfloat16)
    base = GROUP * HD
    dkey = dkey * SCALE
    out_ref[:, base : base + HD] = (dkey * cos - turned(dkey) * sine).astype(jnp.bfloat16)
    out_ref[:, base + HD : base + 2 * HD] = dvalue.astype(jnp.bfloat16)


def per_sequence(kernel, arrays, tables, more, out_width):
    rows = arrays[0].shape[0]

    def by_row(width):
        return pl.BlockSpec((LEN, width), lambda i: (i, 0))

    fixed = [pl.BlockSpec(t.shape, lambda i: (0, 0)) for t in tables]
    return pl.pallas_call(
        kernel,
        grid=(rows // LEN,),
        in_specs=[by_row(a.shape[1]) for a in arrays]
        + fixed
        + [by_row(a.shape[1]) for a in more],
        out_specs=by_row(out_width),
        out_shape=jax.ShapeDtypeStruct((rows, out_width), jnp.bfloat16),
        compiler_params=limited(14),
    )(*arrays, *tables, *more)


def rotary_tables():
    half = HD // 2
    inv_freq = rope_base ** (-(jnp.arange(half).astype(jnp.float32) * 2.0 / HD))
    angles = jnp.arange(LEN).astype(jnp.float32)[:, None] * inv_freq[None, :]
    cos, sine = jnp.cos(angles), jnp.sin(angles)
    return jnp.concatenate([cos, cos], axis=1), jnp.concatenate([-sine, sine], axis=1)


def early_kernel(at_ref, in_own, in_other, cot_own, cot_other, b0, b1, b2, b3, *outs):
    step = pl.program_id(0)
    mine = at_ref[AHEAD + step] < 2
    feat = in_own.shape[1]
    blocks = (b0, b1, b2, b3)
    val_in = jnp.concatenate([b[:, :feat] for b in blocks], axis=0)
    val_cot = jnp.concatenate([b[:, feat:] for b in blocks], axis=0)
    gram_in = nt_dot(jnp.where(mine, in_own[...], in_other[...]), val_in)
    gram_cot = nt_dot(jnp.where(mine, cot_own[...], cot_other[...]), val_cot)
    both = jnp.concatenate([gram_in, gram_cot], axis=1).astype(jnp.bfloat16)
    for d, out in enumerate(outs):

        @pl.when(step == d)
        def _(out=out):
            out[...] = both


def early_grams(inputs, inputs_other, cot, cot_other, blocks, at):
    feat = inputs.shape[1]
    cols = 2 * sum(b.shape[0] for b in blocks)
    sides = (lambda i, t: jnp.minimum(t[AHEAD + i], 1), lambda i, t: jnp.maximum(t[AHEAD + i] - 2, 0))
    plain = [pl.BlockSpec((LEN, feat), lambda i, t, f=f: (f(i, t), 0)) for f in sides]
    shared = [pl.BlockSpec((LEN, feat), lambda i, t, f=f: (f(i, t), t[FEATURE])) for f in sides]
    shape = jax.ShapeDtypeStruct((LEN, cols), jnp.bfloat16)
    return pl.pallas_call(
        early_kernel,
        grid_spec=pltpu.PrefetchScalarGridSpec(
            num_scalar_prefetch=1,
            grid=(4,),
            in_specs=plain
            + shared
            + [pl.BlockSpec(b.shape, lambda i, s: (0, 0)) for b in blocks],
            out_specs=[pl.BlockSpec((LEN, cols), lambda i, s: (0, 0))] * 4,
        ),
        out_shape=[shape] * 4,
        compiler_params=limited(14),
    )(at, inputs, inputs_other, cot, cot_other, *blocks)


def total_of(parts):
    return sum(p.astype(jnp.float32) for p in parts).astype(jnp.bfloat16)


def scores_kernel(at_ref, att_own, att_other, grad_own, grad_other, *refs):
    step = pl.program_id(0)
    mine = at_ref[BEHIND + step] < 2
    blocks, grams, out_ref = refs[:4], refs[4:8], refs[8]
    feat = att_own.shape[1]
    gram = grams[0][...]
    for d in range(1, 4):
        gram = jnp.where(step == d, grams[d][...], gram)
    val_att = jnp.concatenate([b[:, :feat] for b in blocks], axis=0)
    val_grad = jnp.concatenate([b[:, feat:] for b in blocks], axis=0)
    gram_attn = nt_dot(jnp.where(mine, att_own[...], att_other[...]), val_att)
    gram_proj = nt_dot(jnp.where(mine, grad_own[...], grad_other[...]), val_grad)
    cols = gram_attn.shape[1]
    product = gram_attn * gram[:, cols:].astype(jnp.float32)
    product = product + gram_proj * gram[:, :cols].astype(jnp.float32)
    out_ref[...] = jnp.sum(product.reshape(LEN // 8, 8, cols), axis=0)


def sequence_scores(att, att_other, grad, grad_other, blocks, grams, at):
    cols = sum(b.shape[0] for b in blocks)

    def tile(a, first):
        if first:
            return pl.BlockSpec((LEN, a.shape[1]), lambda i, t: (jnp.minimum(t[BEHIND + i], 1), 0))
        return pl.BlockSpec((LEN, a.shape[1]), lambda i, t: (jnp.maximum(t[BEHIND + i] - 2, 0), 0))

    def whole(a):
        return pl.BlockSpec(a.shape, lambda i, s: (0, 0))

    out = pl.pallas_call(
        scores_kernel,
        grid_spec=pltpu.PrefetchScalarGridSpec(
            num_scalar_prefetch=1,
            grid=(4,),
            in_specs=[tile(att, True), tile(att_other, False), tile(grad, True), tile(grad_other, False)]
            + [whole(a) for a in (*blocks, *grams)],
            out_specs=pl.BlockSpec((8, cols), lambda i, t: (t[BEHIND + i], 0)),
        ),
        out_shape=jax.ShapeDtypeStruct((32, cols), jnp.float32),
        compiler_params=limited(18),
    )(at, att, att_other, grad, grad_other, *blocks, *grams)
    return jnp.sum(out.reshape(4, 8, VALS, cols // VALS), axis=(1, 3))


def device_scores(
    cand_ids,
    val_ids,
    inputs,
    cotangent,
    queries,
    key_rows,
    value_rows,
    out_weight,
    val_inputs,
    val_cotangents,
    val_attention,
    val_query_grads,
    val_keyvalue_grads,
):
    y, at = lax.axis_index("y"), positions()
    live = (cand_ids != pad_token).astype(jnp.float32)[:, None]
    val_live = (val_ids != pad_token).astype(jnp.float32)[:, None]

    def val_masked(a):
        return (a.astype(jnp.float32) * val_live).astype(jnp.bfloat16)

    first = jnp.concatenate([val_inputs, val_masked(val_cotangents)], axis=1)
    late = jnp.concatenate(
        [val_attention, val_masked(val_query_grads), val_masked(val_keyvalue_grads)], axis=1
    )
    cot_other = swap(cotangent)
    inputs_other = swap(inputs)

    first = jnp.concatenate(along_z(first), axis=0)
    first = along_y(first, 1)
    parts = early_grams(inputs, inputs_other, cotangent, cot_other, first, at)
    parts = [parts[0], *(shift(parts[d], "x", d) for d in (1, 2, 3))]
    half = total_of(parts)
    gram = total_of([half, lax.ppermute(half, "h", [(0, 1), (1, 0)])])
    grams = [gram, *(shift(gram, "x", d) for d in (1, 2, 3))]

    sums = None
    for s, block in enumerate(along_z(out_weight)):
        blocks = along_y(block, 1 if s % 2 == 0 else -1)
        sums = project(cotangent, cot_other, at, s, blocks, sums)
    mine, other = sums
    received = swap(other)

    tables = rotary_tables()
    qkv = (queries, key_rows, value_rows)
    attended = per_sequence(forward_kernel, qkv, tables, (live,), GROUP * HD)
    attended_other = swap(attended)
    grads = per_sequence(backward_kernel, qkv, tables, (mine, received, live), (GROUP + 2) * HD)
    grads_other = swap(grads)

    late = jnp.concatenate(along_z(late), axis=0)
    late = along_y(late, -1)
    part = sequence_scores(attended, attended_other, grads, grads_other, late, grams, at)

    seqs = part.shape[0] // 2
    mine, other = part[:seqs], part[seqs:]
    across = [
        lax.ppermute(v, ("c", "h"), [(i, i ^ step) for i in range(4)])
        for step, v in ((2, other), (1, mine), (3, other))
    ]
    total = (mine + across[0]) + (across[1] + across[2])
    across = [lax.ppermute(total, "x", [(i, i ^ step) for i in range(4)]) for step in (1, 2, 3)]
    total = (total + across[0]) + (across[1] + across[2])
    slots_of = (0, 2, 3, 1)
    scores = jnp.zeros_like(total)
    for j in range(VALS):
        here = ((y + j) % VALS == jnp.arange(VALS)).astype(jnp.float32)[None, :]
        scores = scores + total[:, slots_of[j]][:, None] * here
    return scores * (1.0 / (64.0 * D))


def solution(mesh):
    finer = Mesh(mesh.devices.reshape(4, 4, 2, 2, 4), (*DP, *TENSOR))
    in_specs = (
        P(DP),
        P(DP),
        P(DP, TENSOR),
        P(DP, None),
        P(DP, TENSOR),
        P(DP, TENSOR),
        P(DP, TENSOR),
        P(TENSOR, DP),
        P(DP, TENSOR),
        P(DP, TENSOR),
        P(DP, TENSOR),
        P(DP, TENSOR),
        P(DP, TENSOR),
    )
    return jax.shard_map(
        device_scores, mesh=finer, in_specs=in_specs, out_specs=P(DP, None), check_vma=False
    )
```
